32 devices in a mesh: rows: 8 (over y, x, core), model: 4 (over z).
Axes of the slice: x: 2, y: 2, z: 4, core: 2. Of those that a mesh axis runs over, the one named last changes fastest.
Arguments:
- weight_gate: bfloat16 [2048, 8192], P('rows', 'model'), may hold values from -0.125 to 0.125
- low_gate: bfloat16 [2048, 64], P('rows'), may hold values from -0.125 to 0.125
- high_gate: bfloat16 [64, 8192], P(None, 'model'), may hold values from -0.75 to 0.75
- weight_up: bfloat16 [2048, 8192], P('rows', 'model'), may hold values from -0.125 to 0.125
- low_up: bfloat16 [2048, 64], P('rows'), may hold values from -0.125 to 0.125
- high_up: bfloat16 [64, 8192], P(None, 'model'), may hold values from -0.75 to 0.75
- weight_down: bfloat16 [8192, 2048], P('model', 'rows'), may hold values from -0.0625 to 0.0625
- low_down: bfloat16 [8192, 64], P('model'), may hold values from -0.0625 to 0.0625
- high_down: bfloat16 [64, 2048], P(None, 'rows'), may hold values from -0.75 to 0.75
- norm_train: float32 [2048], P(('rows', 'model')), may hold values from 0.25 to 1.75
- norm_step: float32 [2048], P(('rows', 'model')), may hold values from -0.3 to 0.3
Outputs:
- final_gate: bfloat16 [8192, 2048], P('model')
- final_up: bfloat16 [8192, 2048], P('model')
- final_down: bfloat16 [2048, 8192], P(None, 'model')
- serve_norm: bfloat16 [2048], replicated
The draws below stay inside these ranges and needn't reach their ends.
All inputs are finite; a program needn't handle non-finite values.
Results may differ from the reference program's by a relative error of at most 0.001.
Values may be sent and summed in bfloat16 or wider, within the bound.
No kernel may reach another device: no remote copies, remote signals or barrier semaphores. Data moves between devices by JAX's collectives and lax.ppermute only.
A program may use at most 192 MiB of HBM per device.

```python
import jax
import jax.numpy as jnp

D_MODEL = 2048
D_INNER = 8192
RANK = 64


def block_scale(own_key, extent, split, least, top_value):
    def one(position, shards_of):
        steps = jax.random.uniform(jax.random.fold_in(jax.random.fold_in(own_key, 6), position), (shards_of,), jnp.float32, least / len(split), top_value / len(split))
        return jnp.repeat(jnp.exp(steps), extent[position] // shards_of).reshape((-1,) + (1,) * (len(extent) - position - 1))

    level = one(*split[0])
    for cut in split[1:]:
        level = level * one(*cut)
    return level


def bell_draw(rng, shape, scale, limit, pieces=(), dtype=jnp.bfloat16):
    drawn = jax.random.normal(rng, shape, jnp.float32) * scale
    if len(pieces) > 0:
        drawn = block_scale(rng, shape, pieces, -0.22, 0.18) * drawn
    return jnp.clip(drawn, min=-limit, max=limit).astype(dtype)


def setup_inputs(seed: int = 0) -> dict:
    keys = jax.random.split(jax.random.key(seed), 12)
    return {
        "weight_gate": bell_draw(keys[0], (D_MODEL, D_INNER), D_MODEL ** -0.5, 0.125, ((0, 8), (1, 4))),
        "low_gate": bell_draw(keys[1], (D_MODEL, RANK), D_MODEL ** -0.5, 0.125, ((0, 8),)),
        "high_gate": bell_draw(keys[2], (RANK, D_INNER), RANK ** -0.5, 0.75, ((1, 4),)),
        "weight_up": bell_draw(keys[3], (D_MODEL, D_INNER), D_MODEL ** -0.5, 0.125, ((0, 8), (1, 4))),
        "low_up": bell_draw(keys[4], (D_MODEL, RANK), D_MODEL ** -0.5, 0.125, ((0, 8),)),
        "high_up": bell_draw(keys[5], (RANK, D_INNER), RANK ** -0.5, 0.75, ((1, 4),)),
        "weight_down": bell_draw(keys[6], (D_INNER, D_MODEL), D_INNER ** -0.5, 0.0625, ((0, 4), (1, 8))),
        "low_down": bell_draw(keys[7], (D_INNER, RANK), D_INNER ** -0.5, 0.0625, ((0, 4),)),
        "high_down": bell_draw(keys[8], (RANK, D_MODEL), RANK ** -0.5, 0.75, ((1, 8),)),
        "norm_train": jnp.clip(1.0 + 0.15 * jax.random.normal(keys[9], (D_MODEL,), jnp.float32), 0.25, 1.75),
        "norm_step": jnp.clip(jax.random.uniform(keys[10], (D_MODEL,), jnp.float32, -0.3, 0.3) * block_scale(keys[10], (D_MODEL,), ((0, 32),), -0.4, 0.0), -0.3, 0.3),
    }


mix_rate = 0.5


def reference(weight_gate, low_gate, high_gate, weight_up, low_up, high_up, weight_down, low_down, high_down, norm_train, norm_step):
    result_gate = weight_gate.astype(jnp.float32) + mix_rate * jnp.dot(low_gate, high_gate, preferred_element_type=jnp.float32)
    result_up = weight_up.astype(jnp.float32) + mix_rate * jnp.dot(low_up, high_up, preferred_element_type=jnp.float32)
    result_down = weight_down.astype(jnp.float32) + mix_rate * jnp.dot(low_down, high_down, preferred_element_type=jnp.float32)
    final_gate = result_gate.T.astype(jnp.bfloat16)
    final_up = result_up.T.astype(jnp.bfloat16)
    final_down = result_down.T.astype(jnp.bfloat16)
    serve_norm = (norm_train + norm_step).astype(jnp.bfloat16)
    return final_gate, final_up, final_down, serve_norm
```

```python
import math

import jax
import jax.numpy as jnp
from jax import lax
from jax.experimental import pallas as pl
from jax.experimental.pallas import tpu as pltpu
from jax.sharding import PartitionSpec as P

mix_rate = 0.5

CORE, X, Y = 1, 2, 4


def merged(weight, low, high):
    return (
        weight.astype(jnp.float32) + mix_rate * jnp.dot(low, high, preferred_element_type=jnp.float32)
    ).astype(jnp.bfloat16)


def flip(array, bit, n_rows):
    return lax.ppermute(array, "rows", [(r, r ^ bit) for r in range(n_rows)])


def place(buffer, pieces, places, out_shape, part, n_parts, tile, rows_first):
    bits = sorted(pieces)
    arrays = [pieces[b] for b in bits]
    width, depth = arrays[0].shape if rows_first else arrays[0].shape[::-1]
    steps = depth // tile
    whole = len(bits) * width == out_shape[1 if rows_first else 0]

    if rows_first:
        in_spec = pl.BlockSpec((width, tile), lambda j, s: (0, j))
    else:
        in_spec = pl.BlockSpec((tile, width), lambda j, s: (j, 0))

    if whole:
        grid = (steps,)
        if rows_first:
            out_spec = pl.BlockSpec((tile, out_shape[1]), lambda j, s: (part * steps + j, 0))
        else:
            out_spec = pl.BlockSpec((out_shape[0], tile), lambda j, s: (0, part * steps + j))

        def body(s, *refs):
            out = refs[-1]
            for b, ref in zip(bits, refs):
                at = pl.ds(pl.multiple_of(s[b] * width, width), width)
                if rows_first:
                    out[:, at] = ref[...].T
                else:
                    out[at, :] = ref[...].T

        in_specs = [in_spec] * len(bits)
    else:
        grid = (steps,)
        raise NotImplementedError

    extra, aliases = [], {}
    if buffer is not None:
        in_specs = in_specs + [pl.BlockSpec(memory_space=pl.ANY)]
        extra = [buffer]
        aliases = {1 + len(bits): 0}
    return pl.pallas_call(
        body,
        out_shape=jax.ShapeDtypeStruct(out_shape, jnp.bfloat16),
        grid_spec=pltpu.PrefetchScalarGridSpec(
            num_scalar_prefetch=1, grid=grid, in_specs=in_specs, out_specs=out_spec
        ),
        input_output_aliases=aliases,
        compiler_params=pltpu.CompilerParams(dimension_semantics=("arbitrary",)),
        name="place",
    )(places, *arrays, *extra)


def place_some(buffer, pieces, places, out_shape, part, tile, rows_first):
    for b, array in sorted(pieces.items()):
        width, depth = array.shape if rows_first else array.shape[::-1]
        steps = depth // tile
        if rows_first:
            in_spec = pl.BlockSpec((width, tile), lambda j, s: (0, j))
            out_spec = pl.BlockSpec((tile, width), lambda j, s, b=b: (part * steps + j, s[b]))
        else:
            in_spec = pl.BlockSpec((tile, width), lambda j, s: (j, 0))
            out_spec = pl.BlockSpec((width, tile), lambda j, s, b=b: (s[b], part * steps + j))

        def body(s, ref, *rest):
            rest[-1][...] = ref[...].T

        specs, extra, aliases = [in_spec], [], {}
        if buffer is not None:
            specs, extra, aliases = [in_spec, pl.BlockSpec(memory_space=pl.ANY)], [buffer], {2: 0}
        buffer = pl.pallas_call(
            body,
            out_shape=jax.ShapeDtypeStruct(out_shape, jnp.bfloat16),
            grid_spec=pltpu.PrefetchScalarGridSpec(
                num_scalar_prefetch=1, grid=(steps,), in_specs=specs, out_specs=out_spec
            ),
            input_output_aliases=aliases,
            compiler_params=pltpu.CompilerParams(dimension_semantics=("arbitrary",)),
            name="place_some",
        )(places, array, *extra)
    return buffer


def gather_norm(own, n_rows, n_model):
    n = own.shape[0]
    at = (lax.axis_index("rows") * n_model + lax.axis_index("model")) * n
    whole = lax.dynamic_update_slice(jnp.zeros((n * n_rows * n_model,), own.dtype), own, (at,))
    for axis, size in (("model", n_model), ("rows", n_rows)):
        step = 1
        while step < size:
            whole = whole + lax.ppermute(whole, axis, [(i, i ^ step) for i in range(size)])
            step *= 2
    return whole


def square(sizes, *args):
    (w_gate, low_gate, high_gate, w_up, low_up, high_up, w_down, low_down, high_down, norm_train, norm_step) = args
    n_rows, n_model = sizes
    places = lax.axis_index("rows").astype(jnp.int32) ^ jnp.arange(n_rows, dtype=jnp.int32)

    def halves(w, low, high, axis):
        n = w.shape[axis] // 2
        out = []
        for h in range(2):
            if axis == 1:
                out.append(merged(w[:, h * n : (h + 1) * n], low, high[:, h * n : (h + 1) * n]))
            else:
                out.append(merged(w[h * n : (h + 1) * n], low[h * n : (h + 1) * n], high))
        return out

    sources = [
        halves(w_gate, low_gate, high_gate, 1),
        halves(w_up, low_up, high_up, 1),
        halves(w_down, low_down, high_down, 0),
    ]
    got = []
    for pair in sources:
        have = [{0: part} for part in pair]
        for part in have:
            part[X] = flip(part[0], X, n_rows)
            part[Y] = flip(part[0], Y, n_rows)
        have[0][X | Y] = flip(have[0][X], Y, n_rows)
        have[1][X | Y] = flip(have[1][Y], X, n_rows)
        for part in have:
            for b in (0, X, Y, X | Y):
                part[b | CORE] = flip(part[b], CORE, n_rows)
        got.append(have)

    inner = w_gate.shape[1]
    width = w_gate.shape[0] * n_rows
    finals = []
    for have, rows_first in zip(got, (True, True, False)):
        shape = (inner, width) if rows_first else (width, inner)
        last = not rows_first
        out = None
        if not last:
            for h in range(2):
                out = place(out, have[h], places, shape, h, 2, 256, rows_first)
        else:
            for bs in ((0, 1), (2, 3), (4, 5), (6, 7)):
                for h in range(2):
                    out = place_some(out, {b: have[h][b] for b in bs}, places, shape, h, 512, rows_first)
        finals.append(out)
    serve_norm = gather_norm((norm_train + norm_step).astype(jnp.bfloat16), n_rows, n_model)
    return (*finals, serve_norm)


def general(sizes, *args):
    (w_gate, low_gate, high_gate, w_up, low_up, high_up, w_down, low_down, high_down, norm_train, norm_step) = args
    finals = [
        lax.all_gather(merged(w, low, high), "rows", axis=axis, tiled=True).T
        for w, low, high, axis in (
            (w_gate, low_gate, high_gate, 0),
            (w_up, low_up, high_up, 0),
            (w_down, low_down, high_down, 1),
        )
    ]
    return (*finals, gather_norm((norm_train + norm_step).astype(jnp.bfloat16), *sizes))


def solution(mesh):
    n_rows, n_model = mesh.shape["rows"], mesh.shape["model"]
    side = math.isqrt(n_rows // 2)
    local = square if side == 2 and 2 * side * side == n_rows else general

    in_specs = (
        P("rows", "model"),
        P("rows", None),
        P(None, "model"),
        P("rows", "model"),
        P("rows", None),
        P(None, "model"),
        P("model", "rows"),
        P("model", None),
        P(None, "rows"),
        P(("rows", "model")),
        P(("rows", "model")),
    )
    out_specs = (P("model", None), P("model", None), P(None, "model"), P())
    return jax.shard_map(
        lambda *args: local((n_rows, n_model), *args),
        mesh=mesh,
        in_specs=in_specs,
        out_specs=out_specs,
        check_vma=False,
    )
```
